32 devices in a mesh: seq: 16 (over z, y, x), bat: 2 (over core).
Axes of the slice: x: 2, y: 2, z: 4, core: 2. Of those that a mesh axis runs over, the one named last changes fastest.
Arguments:
- tokens: bfloat16 [2, 65536, 256], P('bat', 'seq'), may hold values from -6 to 6
- filter_spectrum: bfloat16 [2, 256, 256, 256], P(None, 'seq', None, 'bat'), may hold values from -6 to 6
- skip_gain: float32 [256], replicated, may hold values from 0.5 to 1.5
Outputs:
- mixed: bfloat16 [2, 65536, 256], P('bat', 'seq')
The draws below stay inside these ranges and needn't reach their ends.
All inputs are finite; a program needn't handle non-finite values.
Results may differ from the reference program's by a relative error of at most 0.012.
Values may be sent and summed in bfloat16 or wider, within the bound.
A program may use at most 64 MiB of HBM per device.

```python
import math
import jax
import jax.numpy as jnp
from jax import lax

C = 256
N1 = 256
N2 = 256
BATCH = 2
LENGTH = 65536


def level_of(own_key, shape, pieces, least, largest):
    def one(dim, parts):
        steps = jax.random.uniform(jax.random.fold_in(jax.random.fold_in(own_key, 6), dim), (parts,), jnp.float32, least / len(pieces), largest / len(pieces))
        return jnp.repeat(jnp.exp(steps), shape[dim] // parts).reshape((-1,) + (1,) * (len(shape) - dim - 1))

    gain = one(*pieces[0])
    for cut in pieces[1:]:
        gain = gain * one(*cut)
    return gain


def noise(key, shape, scale, most, shards=(), kind=jnp.bfloat16):
    array = jax.random.normal(key, shape, jnp.float32) * scale
    if len(shards) > 0:
        array = level_of(key, shape, shards, -0.22, 0.18) * array
    return jnp.clip(array, min=-most, max=most).astype(kind)


def setup_inputs(seed: int = 0) -> dict:
    key_of = jax.random.split(jax.random.key(seed), 4)
    return {
        "tokens": noise(key_of[0], (BATCH, LENGTH, C), 1.0, 6.0, ((0, 2), (1, 16))),
        "filter_spectrum": noise(key_of[1], (2, N1, N2, C), 1.0, 6.0, ((1, 16), (3, 2))),
        "skip_gain": jnp.clip(jax.random.uniform(key_of[2], (C,), jnp.float32, 0.5, 1.5), 0.5, 1.5),
    }


def cos_sin(points):
    steps_range = jnp.arange(points, dtype=jnp.int32)
    index_grid = (steps_range[:, None] * steps_range[None, :]) % points
    phase_angle = index_grid.astype(jnp.float32) * (2.0 * math.pi / points)
    return jnp.cos(phase_angle), jnp.sin(phase_angle)


def real_table(points):
    cosine, sine_vals = cos_sin(points)
    return jnp.stack([cosine, -sine_vals], axis=1).astype(jnp.bfloat16)


def complex_table(points, signum, factor):
    cosine, sine_vals = cos_sin(points)
    top_rows = jnp.stack([cosine, signum * sine_vals], axis=1)
    low_rows = jnp.stack([-signum * sine_vals, cosine], axis=1)
    return (jnp.stack([top_rows, low_rows], axis=0) * factor).astype(jnp.bfloat16)


def final_table(points):
    cosine, sine_vals = cos_sin(points)
    return (jnp.stack([cosine, -sine_vals], axis=0) / points).astype(jnp.bfloat16)


def twiddle_phase(first_rows, second_rows, period):
    index_grid = (first_rows[:, None] * second_rows[None, :]) % period
    phase_angle = index_grid.astype(jnp.float32) * (2.0 * math.pi / period)
    return jnp.cos(phase_angle)[..., None], jnp.sin(phase_angle)[..., None]


def round_half(values):
    return lax.optimization_barrier(values.astype(jnp.bfloat16)).astype(jnp.float32)


def reference(tokens, filter_spectrum, skip_gain):
    period = N1 * N2
    forward_rows = real_table(N1).astype(jnp.float32)
    forward_cols = complex_table(N2, -1.0, 1.0).astype(jnp.float32)
    inverse_cols = complex_table(N2, 1.0, 1.0 / N2).astype(jnp.float32)
    inverse_rows = final_table(N1).astype(jnp.float32)
    cos_tw, sin_tw = twiddle_phase(jnp.arange(N1, dtype=jnp.int32), jnp.arange(N2, dtype=jnp.int32), period)
    filters_f32 = filter_spectrum.astype(jnp.float32)

    def one_sequence(sequence):
        columns = sequence.reshape(N1, N2, C).astype(jnp.float32)
        first_section = jnp.einsum("nmc,nsk->skmc", columns, forward_rows)
        real_part = first_section[0] * cos_tw + first_section[1] * sin_tw
        imag_part = first_section[1] * cos_tw - first_section[0] * sin_tw
        turned = round_half(jnp.stack([real_part, imag_part]))
        spectrum = round_half(jnp.einsum("rknc,rnsj->skjc", turned, forward_cols))
        prod_real = spectrum[0] * filters_f32[0] - spectrum[1] * filters_f32[1]
        prod_imag = spectrum[0] * filters_f32[1] + spectrum[1] * filters_f32[0]
        product = round_half(jnp.stack([prod_real, prod_imag]))
        back_section = jnp.einsum("rkjc,rjsn->sknc", product, inverse_cols)
        real_back = back_section[0] * cos_tw - back_section[1] * sin_tw
        imag_back = back_section[0] * sin_tw + back_section[1] * cos_tw
        turned_back = round_half(jnp.stack([real_back, imag_back]))
        filtered = jnp.einsum("rknc,rkm->mnc", turned_back, inverse_rows)
        result = filtered + skip_gain * columns
        return result.astype(jnp.bfloat16).reshape(N1 * N2, C)

    return lax.map(one_sequence, tokens)
```

```python
import functools

import jax
import jax.numpy as jnp
import numpy as np
from jax import lax
from jax.experimental import pallas as pl
from jax.experimental.pallas import tpu as pltpu
from jax.sharding import PartitionSpec as P


def cos_sin(points):
    grid = np.outer(np.arange(points), np.arange(points)) % points
    angle = grid * (2.0 * np.pi / points)
    return np.cos(angle), np.sin(angle)


def tables(n1, n2):
    cos1, sin1 = cos_sin(n1)
    cos2, sin2 = cos_sin(n2)
    first = np.concatenate([cos1, -sin1], axis=0)
    forward = np.block([[cos2, -sin2], [sin2, cos2]])
    back = np.block([[cos2, sin2], [-sin2, cos2]]) / n2
    last = np.concatenate([cos1, -sin1], axis=1) / n1
    theta = np.outer(np.arange(n1), np.arange(n2)) % (n1 * n2) * (2.0 * np.pi / (n1 * n2))
    half = [t.astype(np.float32).astype(jnp.bfloat16) for t in (first, forward, back, last)]
    turn = np.stack([np.cos(theta), np.sin(theta)]).astype(np.float32)
    return (*half, turn)


def convolve(tile, filt_re, filt_im, gain, first, forward, back, last, turn):
    f32, bf16 = jnp.float32, jnp.bfloat16
    n1, n2 = tile.shape
    dot = functools.partial(jnp.dot, preferred_element_type=f32)
    section = dot(first, tile)
    cos_t, sin_t = turn[0], turn[1]
    a_re, a_im = section[:n1], section[n1:]
    turned = jnp.concatenate(
        [(a_re * cos_t + a_im * sin_t).astype(bf16), (a_im * cos_t - a_re * sin_t).astype(bf16)],
        axis=1,
    )
    spectrum = dot(turned, forward).astype(bf16).astype(f32)
    x_re, x_im = spectrum[:, :n2], spectrum[:, n2:]
    f_re, f_im = filt_re.astype(f32), filt_im.astype(f32)
    product = jnp.concatenate(
        [(x_re * f_re - x_im * f_im).astype(bf16), (x_re * f_im + x_im * f_re).astype(bf16)],
        axis=1,
    )
    section = dot(product, back)
    b_re, b_im = section[:, :n2], section[:, n2:]
    turned = jnp.concatenate(
        [(b_re * cos_t - b_im * sin_t).astype(bf16), (b_re * sin_t + b_im * cos_t).astype(bf16)],
        axis=0,
    )
    filtered = dot(last, turned)
    return (filtered + gain * tile.astype(f32)).astype(bf16)


def kernel(tok_ref, filt_ref, gain_ref, first, forward, back, last, turn, out_ref):
    devs, _, rows, n2 = tok_ref.shape
    n1 = devs * rows
    tile = tok_ref[:, 0].reshape(n1, n2)
    filt_re = filt_ref[:, 0, 0].reshape(n1, n2)
    filt_im = filt_ref[:, 0, 1].reshape(n1, n2)
    gain = gain_ref[pl.program_id(0)]
    out = convolve(
        tile, filt_re, filt_im, gain, first[...], forward[...], back[...], last[...], turn[...]
    )
    out_ref[...] = out.reshape(devs, 1, rows, n2)


def body(tokens, filter_spectrum, skip_gain):
    seq = lax.axis_size("seq")
    bats = lax.axis_size("bat")
    me, bat = lax.axis_index("seq"), lax.axis_index("bat")
    sequences, local, channels = tokens.shape
    _, rows, n2, held = filter_spectrum.shape
    n1 = rows * seq
    consts = tables(n1, n2)
    mine = channels // seq
    if sequences == 1 and bats == 2 and held % seq == 0 and rows % 16 == 0:
        part = held // seq
        tok = tokens[0].T.reshape(bats, seq, part, rows, n2).transpose(1, 0, 2, 3, 4)
        tok = tok.reshape(seq, mine, rows, n2)
        fil = filter_spectrum.transpose(3, 0, 1, 2).reshape(seq, part, 2, rows, n2)
        fil = lax.all_to_all(fil, "seq", split_axis=0, concat_axis=0)
        tok = lax.all_to_all(tok, "seq", split_axis=0, concat_axis=0)
        other = lax.ppermute(fil, "bat", [(0, 1), (1, 0)])
        low = jnp.where(bat == 0, fil, other)
        high = jnp.where(bat == 0, other, fil)
        fil = jnp.concatenate([low, high], axis=1)
        gain = lax.dynamic_slice_in_dim(skip_gain.reshape(bats, seq, part), me, 1, axis=1)
        gain = gain.reshape(mine)
        whole = lambda t: pl.BlockSpec(t.shape, lambda c: (0,) * t.ndim)
        out = pl.pallas_call(
            kernel,
            grid=(mine,),
            in_specs=[
                pl.BlockSpec((seq, 1, rows, n2), lambda c: (0, c, 0, 0)),
                pl.BlockSpec((seq, 1, 2, rows, n2), lambda c: (0, c, 0, 0, 0)),
                pl.BlockSpec(memory_space=pltpu.SMEM),
                *[whole(t) for t in consts],
            ],
            out_specs=pl.BlockSpec((seq, 1, rows, n2), lambda c: (0, c, 0, 0)),
            out_shape=jax.ShapeDtypeStruct((seq, mine, rows, n2), jnp.bfloat16),
        )(tok, fil, gain, *[jnp.asarray(t) for t in consts])
        out = lax.all_to_all(out, "seq", split_axis=0, concat_axis=0)
        out = out.reshape(seq, bats, part, local).transpose(1, 0, 2, 3).reshape(channels, local)
        return out.T[None]
    fil = lax.all_gather(filter_spectrum, "bat", axis=3, tiled=True).transpose(0, 3, 1, 2)
    fil = lax.all_to_all(fil, "seq", split_axis=1, concat_axis=2, tiled=True)
    tok = tokens.reshape(sequences, rows, n2, channels).transpose(0, 3, 1, 2)
    tok = lax.all_to_all(tok, "seq", split_axis=1, concat_axis=2, tiled=True)
    gain = lax.dynamic_slice_in_dim(skip_gain, me * mine, mine)
    one = lambda t, f, g: convolve(t, f[0], f[1], g, *[jnp.asarray(t) for t in consts])
    per_channel = jax.vmap(one, in_axes=(0, 1, 0))
    out = jax.vmap(per_channel, in_axes=(0, None, None))(tok, fil, gain)
    out = lax.all_to_all(out, "seq", split_axis=2, concat_axis=1, tiled=True)
    return out.reshape(sequences, channels, local).transpose(0, 2, 1)


def solution(mesh):
    placed = (P("bat", "seq", None), P(None, "seq", None, "bat"), P())
    return jax.shard_map(
        body, mesh=mesh, in_specs=placed, out_specs=P("bat", "seq", None), check_vma=False
    )
```

```python
import functools

import jax
import jax.numpy as jnp
import numpy as np
from jax import lax
from jax.experimental import pallas as pl
from jax.experimental.pallas import tpu as pltpu
from jax.sharding import PartitionSpec as P


def cos_sin(points):
    grid = np.outer(np.arange(points), np.arange(points)) % points
    angle = grid * (2.0 * np.pi / points)
    return np.cos(angle), np.sin(angle)


def tables(n1, n2):
    cos1, sin1 = cos_sin(n1)
    cos2, sin2 = cos_sin(n2)
    first = np.concatenate([cos1, -sin1], axis=0)
    forward = np.block([[cos2, -sin2], [sin2, cos2]])
    back = np.block([[cos2, sin2], [-sin2, cos2]]) / n2
    last = np.concatenate([cos1, -sin1], axis=1) / n1
    theta = np.outer(np.arange(n1), np.arange(n2)) % (n1 * n2) * (2.0 * np.pi / (n1 * n2))
    half = [t.astype(np.float32).astype(jnp.bfloat16) for t in (first, forward, back, last)]
    turn = np.stack([np.cos(theta), np.sin(theta)]).astype(np.float32)
    return (*half, turn)


def convolve(tile, filt_re, filt_im, gain, first, forward, back, last, turn):
    f32, bf16 = jnp.float32, jnp.bfloat16
    n1, n2 = tile.shape
    dot = functools.partial(jnp.dot, preferred_element_type=f32)
    section = dot(first, tile)
    cos_t, sin_t = turn[0], turn[1]
    a_re, a_im = section[:n1], section[n1:]
    turned = jnp.concatenate(
        [(a_re * cos_t + a_im * sin_t).astype(bf16), (a_im * cos_t - a_re * sin_t).astype(bf16)],
        axis=1,
    )
    spectrum = dot(turned, forward).astype(bf16).astype(f32)
    x_re, x_im = spectrum[:, :n2], spectrum[:, n2:]
    f_re, f_im = filt_re.astype(f32), filt_im.astype(f32)
    product = jnp.concatenate(
        [(x_re * f_re - x_im * f_im).astype(bf16), (x_re * f_im + x_im * f_re).astype(bf16)],
        axis=1,
    )
    section = dot(product, back)
    b_re, b_im = section[:, :n2], section[:, n2:]
    turned = jnp.concatenate(
        [(b_re * cos_t - b_im * sin_t).astype(bf16), (b_re * sin_t + b_im * cos_t).astype(bf16)],
        axis=0,
    )
    filtered = dot(last, turned)
    return (filtered + gain * tile.astype(f32)).astype(bf16)


def kernel(
    tok_ref, filt_ref, gain_ref, first, forward, back, last, turn, out_ref,
    held_tok, held_filt, held_out, tok_send, tok_recv, filt_send, filt_recv,
    pair_send, pair_recv, out_send, out_recv,
):
    seq = lax.axis_size("seq")
    me, bat = lax.axis_index("seq"), lax.axis_index("bat")
    groups, _, _, some, rows, n2 = held_tok.shape
    part = groups * some
    n1 = seq * rows
    mate = (me, 1 - bat)
    remote = functools.partial(
        pltpu.make_async_remote_copy, device_id_type=pl.DeviceIdType.MESH
    )

    barrier = pltpu.get_barrier_semaphore()

    @pl.loop(1, seq)
    def _(k):
        peer = (lax.rem(me + k, seq), bat)
        pl.semaphore_signal(
            barrier, inc=1, device_id=peer, device_id_type=pl.DeviceIdType.MESH
        )

    pl.semaphore_signal(barrier, inc=1, device_id=mate, device_id_type=pl.DeviceIdType.MESH)
    pl.semaphore_wait(barrier, seq)

    def wait_bytes(ref, sem):
        pltpu.make_async_copy(ref, ref, sem).wait()

    def pieces(g, d):
        first_channel = d * part + g * some
        return (
            tok_ref.at[:, pl.ds(first_channel, some)],
            filt_ref.at[pl.ds(first_channel, some)],
        )

    @pl.loop(0, groups)
    def _(g):
        tok, filt = pieces(g, me)
        pltpu.make_async_copy(filt, held_filt.at[bat, g, me], filt_recv.at[g]).start()
        pltpu.make_async_copy(tok, held_tok.at[g, me], tok_recv.at[g]).start()

        @pl.loop(1, seq)
        def _(k):
            d = lax.rem(me + k, seq)
            tok, filt = pieces(g, d)
            remote(
                filt, held_filt.at[bat, g, me], filt_send, filt_recv.at[g], device_id=(d, bat)
            ).start()
            remote(tok, held_tok.at[g, me], tok_send, tok_recv.at[g], device_id=(d, bat)).start()

    @pl.loop(0, groups)
    def _(g):
        wait_bytes(held_filt.at[bat, g], filt_recv.at[g])
        remote(
            held_filt.at[bat, g], held_filt.at[bat, g], pair_send, pair_recv.at[g], device_id=mate
        ).start()
        wait_bytes(held_tok.at[g], tok_recv.at[g])
        wait_bytes(held_filt.at[1 - bat, g], pair_recv.at[g])

        @pl.loop(0, 2 * some)
        def _(c):
            h, j = c // some, lax.rem(c, some)
            out = convolve(
                held_tok[g, :, h, j].reshape(n1, n2),
                held_filt[h, g, :, j, 0].reshape(n1, n2),
                held_filt[h, g, :, j, 1].reshape(n1, n2),
                gain_ref[h, me * part + g * some + j],
                first[...], forward[...], back[...], last[...], turn[...],
            )
            held_out[g, :, h, j] = out.reshape(seq, rows, n2)

        mine = out_ref.at[:, pl.ds(me * part + g * some, some)]
        pltpu.make_async_copy(held_out.at[g, me], mine, out_recv).start()

        @pl.loop(1, seq)
        def _(k):
            d = lax.rem(me + k, seq)
            remote(held_out.at[g, d], mine, out_send, out_recv, device_id=(d, bat)).start()

    wait_bytes(held_tok.at[:, pl.ds(0, seq - 1)], tok_send)
    wait_bytes(held_filt.at[0, :, pl.ds(0, seq - 1)], filt_send)
    wait_bytes(held_filt.at[0], pair_send)
    wait_bytes(held_out.at[:, pl.ds(0, seq - 1)], out_send)
    wait_bytes(out_ref, out_recv)


def body(tokens, filter_spectrum, skip_gain):
    seq = lax.axis_size("seq")
    bats = lax.axis_size("bat")
    me = lax.axis_index("seq")
    sequences, local, channels = tokens.shape
    _, rows, n2, held = filter_spectrum.shape
    n1 = rows * seq
    consts = tables(n1, n2)
    mine = channels // seq
    if sequences == 1 and bats == 2 and held % seq == 0 and rows % 16 == 0:
        part = held // seq
        some = 2 if part % 2 == 0 else 1
        groups = part // some
        tok = tokens[0].T.reshape(bats, held, rows, n2)
        fil = filter_spectrum.transpose(3, 0, 1, 2)
        hbm = pl.BlockSpec(memory_space=pltpu.HBM)
        vmem = pl.BlockSpec(memory_space=pltpu.VMEM)
        dma = pltpu.SemaphoreType.DMA
        out = pl.pallas_call(
            kernel,
            in_specs=[hbm, hbm, pl.BlockSpec(memory_space=pltpu.SMEM), *[vmem] * len(consts)],
            out_specs=hbm,
            out_shape=jax.ShapeDtypeStruct((bats, held, rows, n2), jnp.bfloat16),
            scratch_shapes=[
                pltpu.VMEM((groups, seq, bats, some, rows, n2), jnp.bfloat16),
                pltpu.VMEM((bats, groups, seq, some, 2, rows, n2), jnp.bfloat16),
                pltpu.VMEM((groups, seq, bats, some, rows, n2), jnp.bfloat16),
                dma, dma((groups,)), dma, dma((groups,)),
                dma, dma((groups,)), dma, dma,
            ],
            compiler_params=pltpu.CompilerParams(
                collective_id=0, has_side_effects=True, vmem_limit_bytes=48 * 1024 * 1024
            ),
        )(tok, fil, skip_gain.reshape(bats, held), *[jnp.asarray(t) for t in consts])
        return out.reshape(channels, local).T[None]
    fil = lax.all_gather(filter_spectrum, "bat", axis=3, tiled=True).transpose(0, 3, 1, 2)
    fil = lax.all_to_all(fil, "seq", split_axis=1, concat_axis=2, tiled=True)
    tok = tokens.reshape(sequences, rows, n2, channels).transpose(0, 3, 1, 2)
    tok = lax.all_to_all(tok, "seq", split_axis=1, concat_axis=2, tiled=True)
    gain = lax.dynamic_slice_in_dim(skip_gain, me * mine, mine)
    one = lambda t, f, g: convolve(t, f[0], f[1], g, *[jnp.asarray(t) for t in consts])
    per_channel = jax.vmap(one, in_axes=(0, 1, 0))
    out = jax.vmap(per_channel, in_axes=(0, None, None))(tok, fil, gain)
    out = lax.all_to_all(out, "seq", split_axis=2, concat_axis=1, tiled=True)
    return out.reshape(sequences, channels, local).transpose(0, 2, 1)


def solution(mesh):
    placed = (P("bat", "seq", None), P(None, "seq", None, "bat"), P())
    return jax.shard_map(
        body, mesh=mesh, in_specs=placed, out_specs=P("bat", "seq", None), check_vma=False
    )
```

```python
import functools

import jax
import jax.numpy as jnp
import numpy as np
from jax import lax
from jax.experimental import pallas as pl
from jax.experimental.pallas import tpu as pltpu
from jax.sharding import PartitionSpec as P


def cos_sin(points):
    grid = np.outer(np.arange(points), np.arange(points)) % points
    angle = grid * (2.0 * np.pi / points)
    return np.cos(angle), np.sin(angle)


def tables(n1, n2):
    cos1, sin1 = cos_sin(n1)
    cos2, sin2 = cos_sin(n2)
    first = np.concatenate([cos1, -sin1], axis=0)
    forward = np.block([[cos2, -sin2], [sin2, cos2]])
    back = np.block([[cos2, sin2], [-sin2, cos2]]) / n2
    last = np.concatenate([cos1, -sin1], axis=1) / n1
    theta = np.outer(np.arange(n1), np.arange(n2)) % (n1 * n2) * (2.0 * np.pi / (n1 * n2))
    half = [t.astype(np.float32).astype(jnp.bfloat16) for t in (first, forward, back, last)]
    turn = np.stack([np.cos(theta), np.sin(theta)]).astype(np.float32)
    return (*half, turn)


def convolve(tile, filt_re, filt_im, gain, first, forward, back, last, turn):
    f32, bf16 = jnp.float32, jnp.bfloat16
    n1, n2 = tile.shape
    dot = functools.partial(jnp.dot, preferred_element_type=f32)
    section = dot(first, tile)
    cos_t, sin_t = turn[0], turn[1]
    a_re, a_im = section[:n1], section[n1:]
    turned = jnp.concatenate(
        [(a_re * cos_t + a_im * sin_t).astype(bf16), (a_im * cos_t - a_re * sin_t).astype(bf16)],
        axis=1,
    )
    spectrum = dot(turned, forward).astype(bf16).astype(f32)
    x_re, x_im = spectrum[:, :n2], spectrum[:, n2:]
    f_re, f_im = filt_re.astype(f32), filt_im.astype(f32)
    product = jnp.concatenate(
        [(x_re * f_re - x_im * f_im).astype(bf16), (x_re * f_im + x_im * f_re).astype(bf16)],
        axis=1,
    )
    section = dot(product, back)
    b_re, b_im = section[:, :n2], section[:, n2:]
    turned = jnp.concatenate(
        [(b_re * cos_t - b_im * sin_t).astype(bf16), (b_re * sin_t + b_im * cos_t).astype(bf16)],
        axis=0,
    )
    filtered = dot(last, turned)
    return (filtered + gain * tile.astype(f32)).astype(bf16)


def channel_major(raw, wide, turned):
    rows, n2, lanes = raw.shape
    tiles, _, width = wide.shape
    step = 8

    @pl.loop(0, rows)
    def _(r):
        flat = raw[r].astype(jnp.float32).T
        for t in range(tiles):
            wide[t, pl.ds(r, lanes, stride=rows), :] = flat[:, t * width : (t + 1) * width]

    @pl.loop(0, lanes // step)
    def _(q):
        start = pl.multiple_of(q * (step * rows), step * rows)
        for t in range(tiles):
            block = wide[t, pl.ds(start, step * rows), :].astype(turned.dtype)
            turned[pl.ds(q * step, step), :, t * width : (t + 1) * width] = block.reshape(
                step, rows, width
            )


def kernel(
    tok_ref, filt_ref, gain_ref, first, forward, back, last, turn, out_ref,
    raw_tok, raw_filt, wide, own_tok, own_filt, held_tok, held_filt, held_out,
    load_sem, tok_send, tok_recv, filt_send, filt_recv, pair_send, pair_recv, out_send, out_recv,
):
    seq = lax.axis_size("seq")
    me, bat = lax.axis_index("seq"), lax.axis_index("bat")
    groups, _, halves, some, rows, n2 = held_tok.shape
    held = own_tok.shape[1]
    part = groups * some
    n1 = seq * rows
    mate = (me, 1 - bat)
    mesh_id = pl.DeviceIdType.MESH
    remote = functools.partial(pltpu.make_async_remote_copy, device_id_type=mesh_id)

    loads = [pltpu.make_async_copy(filt_ref.at[p], raw_filt.at[p], load_sem.at[p]) for p in range(2)]
    loads += [
        pltpu.make_async_copy(
            tok_ref.at[:, :, pl.ds(h * held, held)], raw_tok.at[h], load_sem.at[2 + h]
        )
        for h in range(halves)
    ]
    for load in loads:
        load.start()

    barrier = pltpu.get_barrier_semaphore()

    @pl.loop(1, seq)
    def _(k):
        peer = (lax.rem(me + k, seq), bat)
        pl.semaphore_signal(barrier, inc=1, device_id=peer, device_id_type=mesh_id)

    pl.semaphore_signal(barrier, inc=1, device_id=mate, device_id_type=mesh_id)

    def wait_bytes(ref, sem):
        pltpu.make_async_copy(ref, ref, sem).wait()

    for p in range(2):
        loads[p].wait()
        channel_major(raw_filt.at[p], wide, own_filt.at[p])
        if p == 0:
            pl.semaphore_wait(barrier, seq)

        @pl.loop(1, seq)
        def _(k):
            d = lax.rem(me + k, seq)
            remote(
                own_filt.at[p, pl.ds(d * part, part)], held_filt.at[bat, p, me],
                filt_send, filt_recv.at[p], device_id=(d, bat),
            ).start()

        held_filt[bat, p, me] = own_filt[p, pl.ds(me * part, part)]

    for h in range(halves):
        loads[2 + h].wait()
        channel_major(raw_tok.at[h], wide, own_tok.at[h])

    @pl.loop(0, groups)
    def _(g):
        @pl.loop(1, seq)
        def _(k):
            d = lax.rem(me + k, seq)
            remote(
                own_tok.at[:, pl.ds(d * part + g * some, some)], held_tok.at[g, me],
                tok_send, tok_recv.at[g], device_id=(d, bat),
            ).start()

        held_tok[g, me] = own_tok[:, pl.ds(me * part + g * some, some)]

    others = pl.ds(0, seq - 1)
    for p in range(2):
        wait_bytes(held_filt.at[bat, p, others], filt_recv.at[p])
        remote(
            held_filt.at[bat, p], held_filt.at[bat, p], pair_send.at[p], pair_recv.at[p],
            device_id=mate,
        ).start()
    for p in range(2):
        wait_bytes(held_filt.at[1 - bat, p], pair_recv.at[p])

    @pl.loop(0, groups)
    def _(g):
        wait_bytes(held_tok.at[g, others], tok_recv.at[g])

        @pl.loop(0, halves * some)
        def _(c):
            h, j = c // some, lax.rem(c, some)
            channel = g * some + j
            out = convolve(
                held_tok[g, :, h, j].reshape(n1, n2),
                held_filt[h, 0, :, channel].reshape(n1, n2),
                held_filt[h, 1, :, channel].reshape(n1, n2),
                gain_ref[h, me * part + channel],
                first[...], forward[...], back[...], last[...], turn[...],
            )
            held_out[g, :, h, j] = out.reshape(seq, rows, n2)

        mine = out_ref.at[:, pl.ds(me * part + g * some, some)]
        pltpu.make_async_copy(held_out.at[g, me], mine, out_recv).start()

        @pl.loop(1, seq)
        def _(k):
            d = lax.rem(me + k, seq)
            remote(held_out.at[g, d], mine, out_send, out_recv, device_id=(d, bat)).start()

    wait_bytes(held_tok.at[:, others], tok_send)
    wait_bytes(held_filt.at[0, :, others], filt_send)
    for p in range(2):
        wait_bytes(held_filt.at[bat, p], pair_send.at[p])
    wait_bytes(held_out.at[:, others], out_send)
    wait_bytes(out_ref, out_recv)


def body(tokens, filter_spectrum, skip_gain):
    seq = lax.axis_size("seq")
    bats = lax.axis_size("bat")
    me = lax.axis_index("seq")
    sequences, local, channels = tokens.shape
    _, rows, n2, held = filter_spectrum.shape
    n1 = rows * seq
    consts = tables(n1, n2)
    mine = channels // seq
    lane = 128
    if sequences == 1 and bats == 2 and held % seq == 0 and rows % 16 == 0 and held % lane == 0 and n2 % lane == 0:
        part = held // seq
        some = 2 if part % 2 == 0 else 1
        groups = part // some
        tok = tokens.reshape(rows, n2, channels)
        hbm = pl.BlockSpec(memory_space=pltpu.HBM)
        vmem = pl.BlockSpec(memory_space=pltpu.VMEM)
        dma = pltpu.SemaphoreType.DMA
        half = lambda shape: pltpu.VMEM(shape, jnp.bfloat16)
        out = pl.pallas_call(
            kernel,
            in_specs=[hbm, hbm, pl.BlockSpec(memory_space=pltpu.SMEM), *[vmem] * len(consts)],
            out_specs=hbm,
            out_shape=jax.ShapeDtypeStruct((bats, held, rows, n2), jnp.bfloat16),
            scratch_shapes=[
                half((bats, rows, n2, held)),
                half((2, rows, n2, held)),
                pltpu.VMEM((n2 // lane, held * rows, lane), jnp.float32),
                half((bats, held, rows, n2)),
                half((2, held, rows, n2)),
                half((groups, seq, bats, some, rows, n2)),
                half((bats, 2, seq, part, rows, n2)),
                half((groups, seq, bats, some, rows, n2)),
                dma((2 + bats,)), dma, dma((groups,)), dma, dma((2,)),
                dma((2,)), dma((2,)), dma, dma,
            ],
            compiler_params=pltpu.CompilerParams(
                collective_id=0, has_side_effects=True, vmem_limit_bytes=48 * 1024 * 1024
            ),
        )(tok, filter_spectrum, skip_gain.reshape(bats, held), *[jnp.asarray(t) for t in consts])
        return out.reshape(channels, local).T[None]
    fil = lax.all_gather(filter_spectrum, "bat", axis=3, tiled=True).transpose(0, 3, 1, 2)
    fil = lax.all_to_all(fil, "seq", split_axis=1, concat_axis=2, tiled=True)
    tok = tokens.reshape(sequences, rows, n2, channels).transpose(0, 3, 1, 2)
    tok = lax.all_to_all(tok, "seq", split_axis=1, concat_axis=2, tiled=True)
    gain = lax.dynamic_slice_in_dim(skip_gain, me * mine, mine)
    one = lambda t, f, g: convolve(t, f[0], f[1], g, *[jnp.asarray(t) for t in consts])
    per_channel = jax.vmap(one, in_axes=(0, 1, 0))
    out = jax.vmap(per_channel, in_axes=(0, None, None))(tok, fil, gain)
    out = lax.all_to_all(out, "seq", split_axis=2, concat_axis=1, tiled=True)
    return out.reshape(sequences, channels, local).transpose(0, 2, 1)


def solution(mesh):
    placed = (P("bat", "seq", None), P(None, "seq", None, "bat"), P())
    return jax.shard_map(
        body, mesh=mesh, in_specs=placed, out_specs=P("bat", "seq", None), check_vma=False
    )
```

```python
import functools

import jax
import jax.numpy as jnp
import numpy as np
from jax import lax
from jax.experimental import pallas as pl
from jax.experimental.pallas import tpu as pltpu
from jax.sharding import PartitionSpec as P


def cos_sin(points):
    grid = np.outer(np.arange(points), np.arange(points)) % points
    angle = grid * (2.0 * np.pi / points)
    return np.cos(angle), np.sin(angle)


def tables(n1, n2):
    cos1, sin1 = cos_sin(n1)
    cos2, sin2 = cos_sin(n2)
    first = np.concatenate([cos1, -sin1], axis=0)
    forward = np.block([[cos2, -sin2], [sin2, cos2]])
    back = np.block([[cos2, sin2], [-sin2, cos2]]) / n2
    last = np.concatenate([cos1, -sin1], axis=1) / n1
    theta = np.outer(np.arange(n1), np.arange(n2)) % (n1 * n2) * (2.0 * np.pi / (n1 * n2))
    half = [t.astype(np.float32).astype(jnp.bfloat16) for t in (first, forward, back, last)]
    turn = np.stack([np.cos(theta), np.sin(theta)]).astype(np.float32)
    return (*half, turn)


def convolve(tile, filt_re, filt_im, gain, first, forward, back, last, turn):
    f32, bf16 = jnp.float32, jnp.bfloat16
    n1, n2 = tile.shape
    dot = functools.partial(jnp.dot, preferred_element_type=f32)
    section = dot(first, tile)
    cos_t, sin_t = turn[0], turn[1]
    a_re, a_im = section[:n1], section[n1:]
    turned = jnp.concatenate(
        [(a_re * cos_t + a_im * sin_t).astype(bf16), (a_im * cos_t - a_re * sin_t).astype(bf16)],
        axis=1,
    )
    spectrum = dot(turned, forward).astype(bf16).astype(f32)
    x_re, x_im = spectrum[:, :n2], spectrum[:, n2:]
    f_re, f_im = filt_re.astype(f32), filt_im.astype(f32)
    product = jnp.concatenate(
        [(x_re * f_re - x_im * f_im).astype(bf16), (x_re * f_im + x_im * f_re).astype(bf16)],
        axis=1,
    )
    section = dot(product, back)
    b_re, b_im = section[:, :n2], section[:, n2:]
    turned = jnp.concatenate(
        [(b_re * cos_t - b_im * sin_t).astype(bf16), (b_re * sin_t + b_im * cos_t).astype(bf16)],
        axis=0,
    )
    filtered = dot(last, turned)
    return (filtered + gain * tile.astype(f32)).astype(bf16)


def channel_major(raw, wide, turned):
    rows, n2, lanes = raw.shape
    tiles, _, width = wide.shape
    step = 8

    @pl.loop(0, rows)
    def _(r):
        flat = raw[r].astype(jnp.float32).T
        for t in range(tiles):
            wide[t, pl.ds(r, lanes, stride=rows), :] = flat[:, t * width : (t + 1) * width]

    @pl.loop(0, lanes // step)
    def _(q):
        start = pl.multiple_of(q * (step * rows), step * rows)
        for t in range(tiles):
            block = wide[t, pl.ds(start, step * rows), :].astype(turned.dtype)
            turned[pl.ds(q * step, step), :, t * width : (t + 1) * width] = block.reshape(
                step, rows, width
            )


def kernel(tok_ref, filt_ref, gain_ref, *refs):
    table_refs, refs = refs[:5], refs[5:]
    out_ref, table_bufs, refs = refs[0], refs[1:6], refs[6:]
    raw_tok, raw_filt, wide, own_tok, own_filt, held_tok, held_filt, held_out = refs[:8]
    load_sem, table_sem, tok_send, tok_recv, filt_send, filt_recv = refs[8:14]
    pair_send, pair_recv, out_send, out_recv = refs[14:]
    first, forward, back, last, turn = table_bufs
    seq = lax.axis_size("seq")
    me, bat = lax.axis_index("seq"), lax.axis_index("bat")
    groups, _, halves, some, rows, n2 = held_tok.shape
    held = own_tok.shape[1]
    part = groups * some
    n1 = seq * rows
    mate = (me, 1 - bat)
    mesh_id = pl.DeviceIdType.MESH
    remote = functools.partial(pltpu.make_async_remote_copy, device_id_type=mesh_id)

    loads = [pltpu.make_async_copy(filt_ref.at[p], raw_filt.at[p], load_sem.at[p]) for p in range(2)]
    loads += [
        pltpu.make_async_copy(
            tok_ref.at[:, :, pl.ds(h * held, held)], raw_tok.at[h], load_sem.at[2 + h]
        )
        for h in range(halves)
    ]
    table_loads = [
        pltpu.make_async_copy(src, dst, table_sem.at[i])
        for i, (src, dst) in enumerate(zip(table_refs, table_bufs))
    ]
    for load in loads + table_loads:
        load.start()

    barrier = pltpu.get_barrier_semaphore()

    @pl.loop(1, seq)
    def _(k):
        peer = (lax.rem(me + k, seq), bat)
        pl.semaphore_signal(barrier, inc=1, device_id=peer, device_id_type=mesh_id)

    pl.semaphore_signal(barrier, inc=1, device_id=mate, device_id_type=mesh_id)

    def wait_bytes(ref, sem):
        pltpu.make_async_copy(ref, ref, sem).wait()

    for p in range(2):
        loads[p].wait()
        channel_major(raw_filt.at[p], wide, own_filt.at[p])
        if p == 0:
            pl.semaphore_wait(barrier, seq)

        @pl.loop(1, seq)
        def _(k):
            d = lax.rem(me + k, seq)
            remote(
                own_filt.at[p, pl.ds(d * part, part)], held_filt.at[bat, p, me],
                filt_send, filt_recv.at[p], device_id=(d, bat),
            ).start()

        held_filt[bat, p, me] = own_filt[p, pl.ds(me * part, part)]

    for h in range(halves):
        loads[2 + h].wait()
        channel_major(raw_tok.at[h], wide, own_tok.at[h])

    @pl.loop(0, groups)
    def _(g):
        @pl.loop(1, seq)
        def _(k):
            d = lax.rem(me + k, seq)
            remote(
                own_tok.at[:, pl.ds(d * part + g * some, some)], held_tok.at[g, me],
                tok_send, tok_recv.at[g], device_id=(d, bat),
            ).start()

        held_tok[g, me] = own_tok[:, pl.ds(me * part + g * some, some)]

    for load in table_loads:
        load.wait()

    others = pl.ds(0, seq - 1)
    for p in range(2):
        wait_bytes(held_filt.at[bat, p, others], filt_recv.at[p])
        remote(
            held_filt.at[bat, p], held_filt.at[bat, p], pair_send.at[p], pair_recv.at[p],
            device_id=mate,
        ).start()
    for p in range(2):
        wait_bytes(held_filt.at[1 - bat, p], pair_recv.at[p])

    @pl.loop(0, groups)
    def _(g):
        wait_bytes(held_tok.at[g, others], tok_recv.at[g])

        @pl.loop(0, halves * some)
        def _(c):
            h, j = c // some, lax.rem(c, some)
            channel = g * some + j
            out = convolve(
                held_tok[g, :, h, j].reshape(n1, n2),
                held_filt[h, 0, :, channel].reshape(n1, n2),
                held_filt[h, 1, :, channel].reshape(n1, n2),
                gain_ref[h, me * part + channel],
                first[...], forward[...], back[...], last[...], turn[...],
            )
            held_out[g, :, h, j] = out.reshape(seq, rows, n2)

        mine = out_ref.at[:, pl.ds(me * part + g * some, some)]
        pltpu.make_async_copy(held_out.at[g, me], mine, out_recv).start()

        @pl.loop(1, seq)
        def _(k):
            d = lax.rem(me + k, seq)
            remote(held_out.at[g, d], mine, out_send, out_recv, device_id=(d, bat)).start()

    wait_bytes(held_tok.at[:, others], tok_send)
    wait_bytes(held_filt.at[0, :, others], filt_send)
    for p in range(2):
        wait_bytes(held_filt.at[bat, p], pair_send.at[p])
    wait_bytes(held_out.at[:, others], out_send)
    wait_bytes(out_ref, out_recv)


def body(tokens, filter_spectrum, skip_gain):
    seq = lax.axis_size("seq")
    bats = lax.axis_size("bat")
    me = lax.axis_index("seq")
    sequences, local, channels = tokens.shape
    _, rows, n2, held = filter_spectrum.shape
    n1 = rows * seq
    consts = tables(n1, n2)
    mine = channels // seq
    lane = 128
    if sequences == 1 and bats == 2 and held % seq == 0 and rows % 16 == 0 and held % lane == 0 and n2 % lane == 0:
        part = held // seq
        some = 2 if part % 2 == 0 else 1
        groups = part // some
        tok = tokens.reshape(rows, n2, channels)
        hbm = pl.BlockSpec(memory_space=pltpu.HBM)
        dma = pltpu.SemaphoreType.DMA
        half = lambda shape: pltpu.VMEM(shape, jnp.bfloat16)
        out = pl.pallas_call(
            kernel,
            in_specs=[hbm, hbm, pl.BlockSpec(memory_space=pltpu.SMEM), *[hbm] * len(consts)],
            out_specs=hbm,
            out_shape=jax.ShapeDtypeStruct((bats, held, rows, n2), jnp.bfloat16),
            scratch_shapes=[
                *[pltpu.VMEM(t.shape, t.dtype) for t in consts],
                half((bats, rows, n2, held)),
                half((2, rows, n2, held)),
                pltpu.VMEM((n2 // lane, held * rows, lane), jnp.float32),
                half((bats, held, rows, n2)),
                half((2, held, rows, n2)),
                half((groups, seq, bats, some, rows, n2)),
                half((bats, 2, seq, part, rows, n2)),
                half((groups, seq, bats, some, rows, n2)),
                dma((2 + bats,)), dma((len(consts),)), dma, dma((groups,)), dma, dma((2,)),
                dma((2,)), dma((2,)), dma, dma,
            ],
            compiler_params=pltpu.CompilerParams(
                collective_id=0, has_side_effects=True, vmem_limit_bytes=66_900_000
            ),
        )(tok, filter_spectrum, skip_gain.reshape(bats, held), *[jnp.asarray(t) for t in consts])
        return out.reshape(channels, local).T[None]
    fil = lax.all_gather(filter_spectrum, "bat", axis=3, tiled=True).transpose(0, 3, 1, 2)
    fil = lax.all_to_all(fil, "seq", split_axis=1, concat_axis=2, tiled=True)
    tok = tokens.reshape(sequences, rows, n2, channels).transpose(0, 3, 1, 2)
    tok = lax.all_to_all(tok, "seq", split_axis=1, concat_axis=2, tiled=True)
    gain = lax.dynamic_slice_in_dim(skip_gain, me * mine, mine)
    one = lambda t, f, g: convolve(t, f[0], f[1], g, *[jnp.asarray(t) for t in consts])
    per_channel = jax.vmap(one, in_axes=(0, 1, 0))
    out = jax.vmap(per_channel, in_axes=(0, None, None))(tok, fil, gain)
    out = lax.all_to_all(out, "seq", split_axis=2, concat_axis=1, tiled=True)
    return out.reshape(sequences, channels, local).transpose(0, 2, 1)


def solution(mesh):
    placed = (P("bat", "seq", None), P(None, "seq", None, "bat"), P())
    return jax.shard_map(
        body, mesh=mesh, in_specs=placed, out_specs=P("bat", "seq", None), check_vma=False
    )
```
